8 devices in a mesh: dom: 2 (over z, y), ens: 4 (over x, core).
Axes of the slice: x: 2, y: 2, z: 1, core: 2. Of those that a mesh axis runs over, the one named last changes fastest.
Arguments:
- ensemble: bfloat16 [128, 1024, 16, 73], P('ens', None, 'dom')
- w_in: bfloat16 [146, 256], replicated
- w_out: bfloat16 [256, 73], replicated
- obs_op: bfloat16 [73, 16], replicated
- obs_val: float32 [1024, 16, 16], P(None, 'dom')
- obs_wt: float32 [1024, 16, 16], P(None, 'dom')
Outputs:
- output: bfloat16 [128, 1024, 16, 73], P('ens', None, 'dom')
All inputs are finite; a program needn't handle non-finite values.
Results may differ from the reference program's by a relative error of at most 0.001.
Values are sent between devices in bfloat16 or wider.
A program may use at most 1 GiB of HBM per device.

```python
import jax
import jax.numpy as jnp
import numpy as np
from jax import lax

MEMBERS = 128
GRID_LAT = 1024
GRID_LON = 16
CHANNELS = 73
HIDDEN = 256
OBS_CH = 16
PATCH_SIDE = 8
LOC_RADIUS = 4
NS_STEPS = 20

WIN_COLS = PATCH_SIDE + 2 * LOC_RADIUS
WIN_OBS = PATCH_SIDE * WIN_COLS * OBS_CH


def setup_inputs(seed: int = 0) -> dict:
    key_list = jax.random.split(jax.random.key(seed), 8)
    base_field = jax.random.normal(key_list[0], (GRID_LAT, GRID_LON, CHANNELS), jnp.float32)
    spread = jax.random.normal(key_list[1], (MEMBERS, GRID_LAT, GRID_LON, CHANNELS), jnp.float32)
    ensemble = (0.7 * base_field[None] + 0.6 * spread).astype(jnp.bfloat16)
    w_state = jax.random.normal(key_list[2], (CHANNELS, HIDDEN), jnp.float32) * CHANNELS ** -0.5
    w_lap = jax.random.normal(key_list[3], (CHANNELS, HIDDEN), jnp.float32) * (20.0 * CHANNELS) ** -0.5
    w_in = jnp.concatenate([w_state, w_lap], axis=0).astype(jnp.bfloat16)
    w_out = (jax.random.normal(key_list[4], (HIDDEN, CHANNELS), jnp.float32) * (0.8 * HIDDEN ** -0.5)).astype(jnp.bfloat16)
    obs_op = (jax.random.normal(key_list[5], (CHANNELS, OBS_CH), jnp.float32) * CHANNELS ** -0.5).astype(jnp.bfloat16)
    obs_val = 0.9 * jax.random.normal(key_list[6], (GRID_LAT, GRID_LON, OBS_CH), jnp.float32)
    wt_scale = (MEMBERS - 1) / (0.5 * (MEMBERS ** 0.5 + WIN_OBS ** 0.5) ** 2)
    obs_wt = wt_scale * jax.random.uniform(key_list[7], (GRID_LAT, GRID_LON, OBS_CH), jnp.float32, 0.25, 1.75)
    return {'ensemble': ensemble, 'w_in': w_in, 'w_out': w_out, 'obs_op': obs_op, 'obs_val': obs_val, 'obs_wt': obs_wt}


def forecast_member(member, w_in, w_out):
    center = member.astype(jnp.float32)
    north_nb = jnp.concatenate([center[:1], center[:-1]], axis=0)
    south_nb = jnp.concatenate([center[1:], center[-1:]], axis=0)
    west_nb = jnp.roll(center, 1, axis=1)
    east_nb = jnp.roll(center, -1, axis=1)
    lap_bf = (north_nb + south_nb + west_nb + east_nb - 4.0 * center).astype(jnp.bfloat16)
    feat_rows = jnp.concatenate([member, lap_bf], axis=-1)
    feat_rows = feat_rows.reshape(GRID_LAT // PATCH_SIDE, PATCH_SIDE * GRID_LON, 2 * CHANNELS)

    def band_mlp(band_feats):
        hidden = jnp.dot(band_feats, w_in, preferred_element_type=jnp.float32)
        act_bf = jax.nn.gelu(hidden).astype(jnp.bfloat16)
        return jnp.dot(act_bf, w_out, preferred_element_type=jnp.float32)

    tendency = lax.map(band_mlp, feat_rows).reshape(GRID_LAT, GRID_LON, CHANNELS)
    return (center + tendency).astype(jnp.bfloat16)


def patch_update(xf_patch, yb_win, yo_win, wt_win):
    eye_mem = jnp.eye(MEMBERS, dtype=jnp.float32)
    x_mean = jnp.mean(xf_patch, axis=0)
    x_anom = xf_patch - x_mean
    y_mean = jnp.mean(yb_win, axis=0)
    y_anom = yb_win - y_mean
    weighted = y_anom * wt_win
    a_matrix = (MEMBERS - 1) * eye_mem + jnp.dot(weighted, y_anom.T)
    trace_a = jnp.trace(a_matrix)

    def ns_step(ns_carry, unused):
        y_mat, z_mat = ns_carry
        t_mat = 0.5 * (3.0 * eye_mem - jnp.dot(z_mat, y_mat))
        return (jnp.dot(y_mat, t_mat), jnp.dot(t_mat, z_mat)), None

    ns_out, unused_out = lax.scan(ns_step, (a_matrix / trace_a, eye_mem), None, length=NS_STEPS)
    s_root = ns_out[1] / jnp.sqrt(trace_a)
    p_ana = jnp.dot(s_root, s_root)
    w_mean = jnp.dot(p_ana, jnp.dot(weighted, yo_win - y_mean))
    t_full = (MEMBERS - 1) ** 0.5 * s_root + w_mean[:, None]
    return x_mean + jnp.einsum('kbc,ke->ebc', x_anom, t_full)


def analysis_band(xf_band, yo_band, wt_band, obs_op):
    n_patch = GRID_LON // PATCH_SIDE
    win_idx = (np.arange(n_patch)[:, None] * PATCH_SIDE - LOC_RADIUS + np.arange(WIN_COLS)[None, :]) % GRID_LON
    xf_f32 = xf_band.astype(jnp.float32)
    ens_obs = jnp.einsum('eync,co->eyno', xf_f32, obs_op.astype(jnp.float32))
    yb_win = jnp.moveaxis(ens_obs[:, :, win_idx, :], 2, 0).reshape(n_patch, MEMBERS, WIN_OBS)
    yo_win = jnp.moveaxis(yo_band[:, win_idx, :], 1, 0).reshape(n_patch, WIN_OBS)
    wt_win = jnp.moveaxis(wt_band[:, win_idx, :], 1, 0).reshape(n_patch, WIN_OBS)
    xf_patch = xf_f32.reshape(MEMBERS, PATCH_SIDE, n_patch, PATCH_SIDE, CHANNELS)
    xf_patch = jnp.transpose(xf_patch, (2, 0, 1, 3, 4)).reshape(n_patch, MEMBERS, PATCH_SIDE * PATCH_SIDE, CHANNELS)
    updated = jax.vmap(patch_update)(xf_patch, yb_win, yo_win, wt_win)
    updated = updated.reshape(n_patch, MEMBERS, PATCH_SIDE, PATCH_SIDE, CHANNELS)
    updated = jnp.transpose(updated, (1, 2, 0, 3, 4)).reshape(MEMBERS, PATCH_SIDE, GRID_LON, CHANNELS)
    return updated.astype(jnp.bfloat16)


def reference(ensemble, w_in, w_out, obs_op, obs_val, obs_wt):
    forecast = lax.map(lambda member: forecast_member(member, w_in, w_out), ensemble)
    n_band = GRID_LAT // PATCH_SIDE
    xf_bands = jnp.moveaxis(forecast.reshape(MEMBERS, n_band, PATCH_SIDE, GRID_LON, CHANNELS), 1, 0)
    yo_bands = obs_val.reshape(n_band, PATCH_SIDE, GRID_LON, OBS_CH)
    wt_bands = obs_wt.reshape(n_band, PATCH_SIDE, GRID_LON, OBS_CH)
    band_out = lax.map(lambda band_args: analysis_band(band_args[0], band_args[1], band_args[2], obs_op), (xf_bands, yo_bands, wt_bands))
    return jnp.moveaxis(band_out, 0, 1).reshape(MEMBERS, GRID_LAT, GRID_LON, CHANNELS)
```

```python
import functools
import math

import jax
import jax.numpy as jnp
from jax import lax
from jax.experimental import pallas as pl
from jax.experimental.pallas import tpu as pltpu
from jax.sharding import PartitionSpec as P

LANES = 128
NS_STEPS = 20
SIDE = 8
CHAN = 73
CHAN_PAD = 80
HIDDEN = 256
N_OBS = 16
MEMBERS = 128
COLS = 8
N_ENS = 4
MEM_DEV = MEMBERS // N_ENS
BANDS_TILE = LANES // SIDE
BANDS_OWN = BANDS_TILE // N_ENS
N_TILES = 37
WIDTH = N_TILES * LANES
OFF_B = 32 * LANES
OFF_C = 36 * LANES
MEM_STEP = 8
CHUNKS = (2, 2, 2, 2)
HIGHEST = lax.Precision.HIGHEST
F32 = jnp.float32
BF16 = jnp.bfloat16
VMEM_LIMIT = 56 * 1024 * 1024


def swap_groups(tiles, lane):
    tiles = list(tiles)
    for s in range(4):
        step = SIDE << s
        low = (lane & step) == 0
        out = list(tiles)
        for i in range(16):
            if i & (1 << s):
                continue
            j = i | (1 << s)
            a, b = tiles[i], tiles[j]
            if s == 3:
                moved = pltpu.roll(jnp.where(low, b, a), step, 1)
                out[i] = jnp.where(low, a, moved)
                out[j] = jnp.where(low, moved, b)
            else:
                out[i] = jnp.where(low, a, pltpu.roll(b, step, 1))
                out[j] = jnp.where(low, pltpu.roll(a, LANES - step, 1), b)
        tiles = out
    return tiles


def gelu_tanh(h):
    root = math.sqrt(2.0 / math.pi)
    inner = h * (root + (root * 0.044715) * (h * h))
    half = 0.5 * h
    return half + half * jnp.tanh(inner)


def forecast_kernel(t0, me_ref, x_ref, prev_ref, next_ref, halo_ref, w1_ref, w2_ref, o0, o1, o2, o3, xs, ns, feat, st, bands):
    tile = t0 + pl.program_id(0)
    rows = CHAN * COLS
    lane = lax.broadcasted_iota(jnp.int32, (1, LANES), 1)
    pad = CHAN_PAD * COLS - rows
    xs[rows:, :] = jnp.zeros((pad, LANES), F32)
    ns[rows:, :] = jnp.zeros((pad, LANES), F32)

    def flat(ref, mi):
        return ref[mi].astype(F32).reshape(rows, LANES)

    def one_member(mi, unused):
        def neighbours(first, last):
            x = flat(x_ref, mi)
            if first:
                north = jnp.where(lane == 0, x, pltpu.roll(x, 1, 1))
            else:
                north = pltpu.roll(jnp.where(lane == LANES - 1, flat(prev_ref, mi), x), 1, 1)
            if last:
                south = jnp.where(lane == LANES - 1, x, pltpu.roll(x, LANES - 1, 1))
            else:
                south = pltpu.roll(jnp.where(lane == 0, flat(next_ref, mi), x), LANES - 1, 1)
            xs[:rows, :] = x
            ns[:rows, :] = north + south

        pl.when(tile == 0)(lambda: neighbours(True, False))
        pl.when(tile == 7)(lambda: neighbours(False, True))
        pl.when((tile > 0) & (tile < 7))(lambda: neighbours(False, False))

        def col(ref, c):
            return ref[pl.ds(c, CHAN_PAD, stride=COLS), :]

        for c in range(COLS):
            west = halo_ref[mi, 0].astype(F32) if c == 0 else col(xs, c - 1)
            east = halo_ref[mi, 1].astype(F32) if c == COLS - 1 else col(xs, c + 1)
            center = col(xs, c)
            lap = col(ns, c) + west + east - 4.0 * center
            feat[:CHAN_PAD, c * LANES:(c + 1) * LANES] = center.astype(BF16)
            feat[CHAN_PAD:, c * LANES:(c + 1) * LANES] = lap.astype(BF16)
        for blk in range(COLS // 2):
            hid = jnp.dot(w1_ref[...], feat[:, blk * 256:(blk + 1) * 256], preferred_element_type=F32)
            act = gelu_tanh(hid).astype(BF16)
            tend = jnp.dot(w2_ref[...], act, preferred_element_type=F32)
            for cc in range(2):
                c = 2 * blk + cc
                xf = col(xs, c) + tend[:, cc * LANES:(cc + 1) * LANES]
                st[c, pl.ds(mi, CHAN_PAD, stride=MEM_STEP), :] = xf
        return unused

    lax.fori_loop(0, MEM_STEP, one_member, 0)

    def grab(ch, c):
        return st[c, ch * MEM_STEP:(ch + 1) * MEM_STEP, :]

    def put(tiles, off):
        for b, tile_b in enumerate(swap_groups(tiles, lane)):
            bands[b, :, pl.ds(pl.multiple_of(off, LANES), LANES)] = tile_b.astype(BF16)

    def one_col(c, unused):
        for g in range(4):
            put([grab(g * 16 + i, c) for i in range(16)], c * 512 + g * LANES)
        return unused

    lax.fori_loop(0, COLS, one_col, 0)

    def one_pair(p, unused):
        put([grab(64 + i % 8, 2 * p + i // 8) for i in range(16)], OFF_B + p * LANES)
        return unused

    lax.fori_loop(0, COLS // 2, one_pair, 0)
    zero = jnp.zeros((MEM_STEP, LANES), F32)
    put([grab(CHAN - 1, c) for c in range(COLS)] + [zero] * 8, OFF_C)
    me = me_ref[0]
    for s, out in enumerate((o0, o1, o2, o3)):
        dest = lax.rem(me + s, N_ENS)
        for j in range(BANDS_OWN):
            out[j] = bands[dest * BANDS_OWN + j]


def forecast(me, xt, halo, w1, w2, t0, nt):
    blk = (MEM_STEP, CHAN, COLS, LANES)
    last = xt.shape[3] // LANES - 1
    out = jax.ShapeDtypeStruct((nt * BANDS_OWN, MEM_DEV, WIDTH), BF16)
    out_spec = pl.BlockSpec((BANDS_OWN, MEM_STEP, WIDTH), lambda t, m: (t, m, 0))
    points = MEM_DEV * nt * LANES * COLS
    return pl.pallas_call(
        functools.partial(forecast_kernel, t0),
        out_shape=[out] * N_ENS,
        grid=(nt, MEM_DEV // MEM_STEP),
        in_specs=[
            pl.BlockSpec(memory_space=pltpu.SMEM),
            pl.BlockSpec(blk, lambda t, m: (m, 0, 0, t0 + t)),
            pl.BlockSpec(blk, lambda t, m: (m, 0, 0, jnp.maximum(t0 + t - 1, 0))),
            pl.BlockSpec(blk, lambda t, m: (m, 0, 0, jnp.minimum(t0 + t + 1, last))),
            pl.BlockSpec((MEM_STEP, 2, CHAN_PAD, LANES), lambda t, m: (m, 0, 0, t)),
            pl.BlockSpec((HIDDEN, 2 * CHAN_PAD), lambda t, m: (0, 0)),
            pl.BlockSpec((CHAN_PAD, HIDDEN), lambda t, m: (0, 0)),
        ],
        out_specs=[out_spec] * N_ENS,
        scratch_shapes=[
            pltpu.VMEM((CHAN_PAD * COLS, LANES), F32),
            pltpu.VMEM((CHAN_PAD * COLS, LANES), F32),
            pltpu.VMEM((2 * CHAN_PAD, COLS * LANES), BF16),
            pltpu.VMEM((COLS, CHAN_PAD * MEM_STEP, LANES), F32),
            pltpu.VMEM((BANDS_TILE, MEM_STEP, WIDTH), BF16),
        ],
        compiler_params=pltpu.CompilerParams(vmem_limit_bytes=VMEM_LIMIT),
        cost_estimate=pl.CostEstimate(flops=points * 112128 * 2, bytes_accessed=points * 73 * 8, transcendentals=0),
        name="forecast",
    )(me, xt, xt, xt, halo, w1, w2)


def split3(a):
    a1 = a.astype(BF16)
    rest = a - a1.astype(F32)
    a2 = rest.astype(BF16)
    return a1, a2, (rest - a2.astype(F32)).astype(BF16)


def gather_members(refs, dst):
    for s, ref in enumerate(refs):
        dst[s * MEM_DEV:(s + 1) * MEM_DEV, :] = ref[0]


def gram_kernel(dom_ref, r0, r1, r2, r3, wc_ref, yo_ref, wt_ref, out_ref, xf, yp_all, cm_all, d_all):
    gather_members((r0, r1, r2, r3), xf)
    for c in range(COLS):
        lhs = jnp.concatenate(
            [xf[:, c * 512:(c + 1) * 512], xf[:, OFF_B + (c // 2) * LANES:OFF_B + (c // 2 + 1) * LANES], xf[:, OFF_C:]], axis=1)
        yb = jnp.dot(lhs, wc_ref[c], preferred_element_type=F32)
        mean = jnp.sum(yb, axis=0, keepdims=True) * (1.0 / MEMBERS)
        anom = yb - mean
        span = slice(c * LANES, (c + 1) * LANES)
        yp_all[:, span] = anom
        cm_all[:, span] = anom * wt_ref[0, c:c + 1, :]
        d_all[:, span] = jnp.broadcast_to(yo_ref[0, c:c + 1, :] - mean, (8, LANES))
    dims = (((1,), (1,)), ((), ()))
    out_ref[0, 0, :MEMBERS, :] = lax.dot_general(cm_all[...], yp_all[...], dims, precision=HIGHEST, preferred_element_type=F32)
    out_ref[0, 0, MEMBERS:, :] = lax.dot_general(d_all[...], cm_all[...], dims, precision=HIGHEST, preferred_element_type=F32)


def band_index(h, i, dom_ref):
    dom = dom_ref[0]
    return 2 * i + (1 - h) * (1 - dom) + h * dom


def gram(dom, pieces, wc, yo, wt):
    nb = pieces[0].shape[0]
    piece = pl.BlockSpec((1, MEM_DEV, WIDTH), lambda h, i, d: (band_index(h, i, d), 0, 0))
    obs = pl.BlockSpec((1, COLS, LANES), lambda h, i, d: (band_index(h, i, d), 0, 0))
    return pl.pallas_call(
        gram_kernel,
        out_shape=jax.ShapeDtypeStruct((2, nb // 2, MEMBERS + 8, MEMBERS), F32),
        grid_spec=pltpu.PrefetchScalarGridSpec(
            num_scalar_prefetch=1,
            grid=(2, nb // 2),
            in_specs=[piece] * N_ENS + [pl.BlockSpec(wc.shape, lambda h, i, d: (0, 0, 0)), obs, obs],
            out_specs=pl.BlockSpec((1, 1, MEMBERS + 8, MEMBERS), lambda h, i, d: (h, i, 0, 0)),
            scratch_shapes=[
                pltpu.VMEM((MEMBERS, WIDTH), BF16),
                pltpu.VMEM((MEMBERS, COLS * LANES), F32),
                pltpu.VMEM((MEMBERS, COLS * LANES), F32),
                pltpu.VMEM((8, COLS * LANES), F32),
            ],
        ),
        compiler_params=pltpu.CompilerParams(vmem_limit_bytes=VMEM_LIMIT),
        cost_estimate=pl.CostEstimate(flops=nb * 2 * 128 * 128 * 1024 * 12, bytes_accessed=nb * 128 * WIDTH * 2, transcendentals=0),
        name="gram",
    )(dom, *pieces, wc, yo, wt)


def ns_kernel(mine_ref, theirs_ref, out_ref):
    n = mine_ref.shape[0]
    row = lax.broadcasted_iota(jnp.int32, (MEMBERS, MEMBERS), 0)
    colm = lax.broadcasted_iota(jnp.int32, (MEMBERS, MEMBERS), 1)
    eye = jnp.where(row == colm, 1.0, 0.0).astype(F32)

    def mm(a, b):
        a1, a2, a3 = a
        b1, b2, b3 = b
        left = jnp.concatenate([jnp.concatenate([a1, a1], axis=1), jnp.concatenate([a2, a2], axis=1)], axis=0)
        high = jnp.dot(left, jnp.concatenate([b1, b2], axis=0), preferred_element_type=F32)
        cross = jnp.dot(jnp.concatenate([a1, a3], axis=1), jnp.concatenate([b3, b1], axis=0), preferred_element_type=F32)
        return high[:a1.shape[0]] + (high[a1.shape[0]:] + cross)

    traces, start = [], []
    for i in range(n):
        a_mat = mine_ref[i, :MEMBERS, :] + theirs_ref[i, :MEMBERS, :] + (MEMBERS - 1.0) * eye
        tr = jnp.sum(jnp.sum(a_mat * eye, axis=1, keepdims=True), axis=0, keepdims=True)
        traces.append(tr)
        start += [a_mat / tr, eye]

    def step(unused, carry):
        parts = [split3(m) for m in carry]
        us = [split3(0.5 * (3.0 * eye - mm(parts[2 * i + 1], parts[2 * i]))) for i in range(n)]
        out = []
        for i in range(n):
            out += [mm(parts[2 * i], us[i]), mm(us[i], parts[2 * i + 1])]
        return tuple(out)

    final = lax.fori_loop(0, NS_STEPS, step, tuple(start))
    for i in range(n):
        s_mat = final[2 * i + 1] / jnp.sqrt(traces[i])
        s_parts = split3(s_mat)
        pa = mm(s_parts, s_parts)
        innov = mine_ref[i, MEMBERS:, :] + theirs_ref[i, MEMBERS:, :]
        wbar = mm(split3(innov), split3(pa))[0:1, :]
        t_mat = math.sqrt(MEMBERS - 1.0) * s_mat + wbar
        short = (1.0 - jnp.sum(t_mat, axis=1, keepdims=True)) * (1.0 / MEMBERS)
        out_ref[i] = t_mat + short


def newton(mine, theirs):
    n = mine.shape[0]
    vm = pl.BlockSpec(memory_space=pltpu.VMEM)
    return pl.pallas_call(
        ns_kernel,
        out_shape=jax.ShapeDtypeStruct((n, MEMBERS, MEMBERS), F32),
        in_specs=[vm, vm],
        out_specs=vm,
        compiler_params=pltpu.CompilerParams(vmem_limit_bytes=VMEM_LIMIT),
        cost_estimate=pl.CostEstimate(flops=n * 60 * 2 * 128 ** 3 * 12, bytes_accessed=n * 3 * 65536, transcendentals=0),
        name="newton",
    )(mine, theirs)


def apply_kernel(dom_ref, t_ref, r0, r1, r2, r3, q0, q1, q2, q3, xf):
    gather_members((r0, r1, r2, r3), xf)
    t1, t2, t3 = split3(t_ref[0, 0])
    for lo in range(0, WIDTH, 512):
        span = slice(lo, min(lo + 512, WIDTH))
        x = xf[:, span]
        acc = jnp.dot(t1, x, preferred_element_type=F32)
        acc = acc + (jnp.dot(t2, x, preferred_element_type=F32) + jnp.dot(t3, x, preferred_element_type=F32))
        out = acc.astype(BF16)
        for s, q in enumerate((q0, q1, q2, q3)):
            q[0, :, span] = out[s * MEM_DEV:(s + 1) * MEM_DEV, :]


def apply_transform(dom, t_all, pieces):
    nb = pieces[0].shape[0]
    piece = pl.BlockSpec((1, MEM_DEV, WIDTH), lambda h, i, d: (band_index(h, i, d), 0, 0))
    return pl.pallas_call(
        apply_kernel,
        out_shape=[jax.ShapeDtypeStruct(pieces[0].shape, BF16)] * N_ENS,
        grid_spec=pltpu.PrefetchScalarGridSpec(
            num_scalar_prefetch=1,
            grid=(2, nb // 2),
            in_specs=[pl.BlockSpec((1, 1, MEMBERS, MEMBERS), lambda h, i, d: (h, i, 0, 0))] + [piece] * N_ENS,
            out_specs=[piece] * N_ENS,
            scratch_shapes=[pltpu.VMEM((MEMBERS, WIDTH), BF16)],
        ),
        compiler_params=pltpu.CompilerParams(vmem_limit_bytes=VMEM_LIMIT),
        cost_estimate=pl.CostEstimate(flops=nb * 2 * 128 * 128 * WIDTH * 3, bytes_accessed=nb * 256 * WIDTH * 2, transcendentals=0),
        name="apply",
    )(dom, t_all, *pieces)


def unpack_kernel(me_ref, q0, q1, q2, q3, *rest):
    out_ref, bands, st = rest[-3:]
    lane = lax.broadcasted_iota(jnp.int32, (1, LANES), 1)
    me = me_ref[0]
    for s, q in enumerate((q0, q1, q2, q3)):
        owner = lax.rem(me + s, N_ENS)
        for j in range(BANDS_OWN):
            bands[owner * BANDS_OWN + j] = q[j]
    per_member = CHAN * COLS

    def fetch(off):
        return swap_groups(
            [bands[b, :, pl.ds(pl.multiple_of(off, LANES), LANES)].astype(F32) for b in range(BANDS_TILE)], lane)

    def put(tile, ch, c):
        st[pl.ds(ch * COLS + c, MEM_STEP, stride=per_member), :] = tile

    def one_col(c, unused):
        for g in range(4):
            for i, tile in enumerate(fetch(c * 512 + g * LANES)):
                put(tile, g * 16 + i, c)
        return unused

    lax.fori_loop(0, COLS, one_col, 0)

    def one_pair(p, unused):
        for i, tile in enumerate(fetch(OFF_B + p * LANES)):
            put(tile, 64 + i % 8, 2 * p + i // 8)
        return unused

    lax.fori_loop(0, COLS // 2, one_pair, 0)
    for c, tile in enumerate(fetch(OFF_C)[:COLS]):
        put(tile, CHAN - 1, c)
    for m in range(MEM_STEP):
        out_ref[m] = st[m * per_member:(m + 1) * per_member, :].reshape(CHAN, COLS, LANES).astype(BF16)


def unpack(me, pieces, total, shape, t0):
    nt = pieces[0].shape[0] // BANDS_OWN
    piece = pl.BlockSpec((BANDS_OWN, MEM_STEP, WIDTH), lambda t, m: (t, m, 0))
    operands = [me, *pieces]
    in_specs = [pl.BlockSpec(memory_space=pltpu.SMEM)] + [piece] * N_ENS
    aliases = {}
    if total is not None:
        operands.append(total)
        in_specs.append(pl.BlockSpec(memory_space=pl.ANY))
        aliases = {len(operands) - 1: 0}
    return pl.pallas_call(
        unpack_kernel,
        out_shape=jax.ShapeDtypeStruct(shape, BF16),
        grid=(nt, MEM_DEV // MEM_STEP),
        in_specs=in_specs,
        out_specs=pl.BlockSpec((MEM_STEP, CHAN, COLS, LANES), lambda t, m: (m, 0, 0, t0 + t)),
        scratch_shapes=[
            pltpu.VMEM((BANDS_TILE, MEM_STEP, WIDTH), BF16),
            pltpu.VMEM((MEM_STEP * CHAN * COLS, LANES), F32),
        ],
        input_output_aliases=aliases,
        compiler_params=pltpu.CompilerParams(vmem_limit_bytes=VMEM_LIMIT),
        cost_estimate=pl.CostEstimate(flops=nt * 20_000_000_000 // 8, bytes_accessed=nt * 9_600_000, transcendentals=0),
        name="unpack",
    )(*operands)


def obs_weights(obs_op):
    eye = jnp.eye(SIDE, dtype=BF16)

    def spread(h_rows):
        return (h_rows[:, None, None, :] * eye[None, :, :, None]).reshape(h_rows.shape[0] * SIDE, SIDE * N_OBS)

    part_a = spread(obs_op[:64])
    part_b = spread(obs_op[64:72])
    part_c = spread(obs_op[72:])
    zeros = jnp.zeros((64, SIDE * N_OBS), BF16)
    out = []
    for c in range(COLS):
        b_rows = jnp.concatenate([part_b, zeros] if c % 2 == 0 else [zeros, part_b], axis=0)
        c_rows = jnp.pad(part_c, ((c * SIDE, LANES - (c + 1) * SIDE), (0, 0)))
        out.append(jnp.concatenate([part_a, b_rows, c_rows], axis=0))
    return jnp.stack(out)


def solution(mesh):
    n_dom, n_ens = mesh.shape['dom'], mesh.shape['ens']
    assert (n_dom, n_ens) == (2, N_ENS)

    def local_cycle(ensemble, w_in, w_out, obs_op, obs_val, obs_wt):
        n_lat = ensemble.shape[1]
        me = lax.axis_index('ens')
        me_arr = me.astype(jnp.int32).reshape(1)
        dom_arr = lax.axis_index('dom').astype(jnp.int32).reshape(1)
        xt = jnp.transpose(ensemble, (0, 3, 2, 1))
        grow = ((0, 0), (0, CHAN_PAD - CHAN))
        w1 = jnp.concatenate([jnp.pad(w_in[:CHAN].T, grow), jnp.pad(w_in[CHAN:].T, grow)], axis=1)
        w2 = jnp.pad(w_out.T, ((0, CHAN_PAD - CHAN), (0, 0)))
        wc = obs_weights(obs_op)

        def own_obs(arr):
            arr = arr.reshape(n_lat // LANES, n_ens, BANDS_OWN, SIDE, COLS, N_OBS)
            arr = lax.dynamic_index_in_dim(arr, me, axis=1, keepdims=False)
            return jnp.transpose(arr, (0, 1, 3, 2, 4)).reshape(-1, COLS, SIDE * N_OBS)

        yo, wt = own_obs(obs_val), own_obs(obs_wt)

        def shift(arr, by):
            return lax.ppermute(arr, 'ens', perm=[(i, (i + by) % n_ens) for i in range(n_ens)])

        def swap_dom(arr):
            return lax.ppermute(arr, 'dom', perm=[(0, 1), (1, 0)])

        starts = [sum(CHUNKS[:k]) for k in range(len(CHUNKS))]
        total = None
        for t0, nt in zip(starts, CHUNKS):
            span = slice(t0 * LANES, (t0 + nt) * LANES)
            edge = jnp.stack([xt[:, :, COLS - 1, span], xt[:, :, 0, span]], axis=1)
            halo = swap_dom(jnp.pad(edge, ((0, 0), (0, 0), (0, CHAN_PAD - CHAN), (0, 0))))
            sent = forecast(me_arr, xt, halo, w1, w2, t0, nt)
            got = [sent[0]] + [shift(sent[s], s) for s in range(1, N_ENS)]
            rows = slice(t0 * BANDS_OWN, (t0 + nt) * BANDS_OWN)
            partial = gram(dom_arr, got, wc, yo[rows], wt[rows])
            t_mine = newton(partial[1], swap_dom(partial[0]))
            t_all = jnp.stack([swap_dom(t_mine), t_mine])
            done = apply_transform(dom_arr, t_all, got)
            back = [done[0]] + [shift(done[s], -s) for s in range(1, N_ENS)]
            total = unpack(me_arr, back, total, xt.shape, t0)
        return jnp.transpose(total, (0, 3, 2, 1))

    state_spec = P('ens', None, 'dom', None)
    obs_spec = P(None, 'dom', None)
    return jax.shard_map(local_cycle, mesh=mesh, in_specs=(state_spec, P(), P(), P(), obs_spec, obs_spec), out_specs=state_spec, check_vma=False)
```
